256 devices in a mesh: lev: 2 (over core), wa: 128 (over y, z, x).
Axes of the slice: x: 4, y: 4, z: 8, core: 2. Of those that a mesh axis runs over, the one named last changes fastest.
Arguments:
- spectral: bfloat16 [1280, 1280, 2, 64], P('wa', None, None, 'lev'), parts along dimension 3, may hold values from -0.15625 to 0.15625
- legendre: bfloat16 [1280, 1280, 384], P('wa'), may hold values from -0.15625 to 0.15625
- wavenumber: int32 [1280], P('wa'), may hold values from 0 to 1279, each once
Outputs:
- grid: float32 [768, 2560, 64], P('wa', None, 'lev'), parts along dimension 2
The draws below stay inside these ranges and needn't reach their ends.
There are 2 independent parts, one for each index of `lev`. The reference program is written for one: setup_inputs(seed, part) draws one part's arguments, and reference() takes and returns one part's arrays. A program takes and returns all parts, laid end to end along the dimension named above; an argument that names none is the same for every part. Nothing has to cross between parts.
Inputs may be any that keep to these rules, and one draw needn't show every extreme that they name: wavenumber names every number of 0 to 1279 exactly once; slot k of spectral and legendre belongs to wavenumber[k].
All inputs are finite; a program needn't handle non-finite values.
Results may differ from the reference program's by a relative error of at most 0.0003.
Values sent between devices are 32-bit elements.
A program may use at most 128 MiB of HBM per device.

```python
import jax
import jax.numpy as jnp
from jax import lax

TRUNC = 1279
NLON = 2560
LEVELS = 32
WAVES = 1280
NORTH = 384


def level_of(stream_key, dims, shards, low, high):
    def one(axis_at, shards_of):
        heights = jax.random.uniform(jax.random.fold_in(jax.random.fold_in(stream_key, 6), axis_at), (shards_of,), jnp.float32, low / len(shards), high / len(shards))
        return jnp.repeat(jnp.exp(heights), dims[axis_at] // shards_of).reshape((-1,) + (1,) * (len(dims) - axis_at - 1))

    factor_of = one(*shards[0])
    for cut in shards[1:]:
        factor_of = factor_of * one(*cut)
    return factor_of


def scatter_about(rng, shape, deviation, limit, cuts=(), kind=jnp.bfloat16):
    values = deviation * jax.random.normal(rng, shape, jnp.float32)
    if cuts:
        values = values * level_of(rng, shape, cuts, -0.22, 0.18)
    return jnp.clip(values, -limit, limit).astype(kind)


def setup_inputs(seed: int = 0, part: int = 0) -> dict:
    streams_of = jax.random.split(jax.random.key(seed), 4)
    own_keys = jax.random.split(jax.random.fold_in(streams_of[3], part), 4)
    return {
        "spectral": scatter_about(own_keys[0], (WAVES, WAVES, 2, LEVELS), (TRUNC + 1) ** -0.5, 0.15625, ((0, 128),)),
        "legendre": scatter_about(streams_of[1], (WAVES, WAVES, NORTH), (TRUNC + 1) ** -0.5, 0.15625, ((0, 128),)),
        "wavenumber": jax.random.permutation(streams_of[2], TRUNC + 1).astype(jnp.int32),
    }


def reference(spectral, legendre, wavenumber):
    degrees = spectral.shape[1]
    levels = spectral.shape[3]
    row_index = jnp.arange(degrees, dtype=jnp.int32)

    def one_slot(slot_item):
        rows_table, coeffs, slot_wave = slot_item
        coeff_rows = coeffs.reshape(degrees, 2 * levels)
        kept = jnp.where((row_index >= slot_wave)[:, None], coeff_rows, jnp.zeros_like(coeff_rows))
        flipped = jnp.where(((row_index - slot_wave) % 2 == 0)[:, None], kept, -kept)
        north_sums = jnp.dot(rows_table.T, kept, preferred_element_type=jnp.float32)
        south_sums = jnp.dot(rows_table.T, flipped, preferred_element_type=jnp.float32)
        return jnp.concatenate([north_sums, south_sums[::-1]], 0)

    fourier = lax.map(one_slot, (legendre, spectral, wavenumber))
    real_part = fourier[..., :levels]
    imag_part = fourier[..., levels:] * (wavenumber != 0).astype(fourier.dtype)[:, None, None]
    complex_coeffs = lax.complex(real_part, imag_part)
    spectrum = jnp.zeros((NLON // 2 + 1,) + real_part.shape[1:], complex_coeffs.dtype)
    spectrum = spectrum.at[wavenumber].set(complex_coeffs)
    gridded = jnp.fft.irfft(spectrum, n=NLON, axis=0) * NLON
    return jnp.transpose(gridded, (1, 0, 2)).astype(jnp.float32)
```

```python
import functools
import math

import jax
import jax.numpy as jnp
from jax import lax
from jax.experimental import pallas as pl
from jax.experimental.pallas import tpu as pltpu
from jax.sharding import PartitionSpec as P

NLON = 2560
LANES = 128
MESH = pl.DeviceIdType.MESH


def kernel(
    dims,
    spec_hbm,
    leg_hbm,
    wave_smem,
    out_ref,
    spec,
    leg,
    turned,
    send,
    recv,
    wave_send,
    wave_recv,
    wave_trig,
    table_hi,
    table_lo,
    xs,
    acc,
    spec_sem,
    leg_sem,
    wave_send_sem,
    wave_recv_sem,
    send_sem,
    recv_sem,
):
    devices, slots, degrees, north, columns, rows = dims
    pairs = slots // 2
    half = devices // 2
    levels = columns // 2
    lev = lax.axis_index("lev")
    me = lax.axis_index("wa")

    spec_copy = pltpu.make_async_copy(spec_hbm, spec, spec_sem)
    spec_copy.start()

    def leg_copy(s):
        return pltpu.make_async_copy(leg_hbm.at[pl.ds(2 * s, 2)], leg.at[pl.ds(2 * s, 2)], leg_sem.at[s])

    for s in range(pairs):
        leg_copy(s).start()

    barrier = pltpu.get_barrier_semaphore()

    def greet(i, carry):
        pl.semaphore_signal(barrier, inc=1, device_id=(lev, lax.rem(me + i, devices)), device_id_type=MESH)
        return carry

    lax.fori_loop(1, devices, greet, 0)

    lane_row = lax.broadcasted_iota(jnp.int32, (1, LANES), 1)
    own_waves = jnp.zeros((1, LANES), jnp.float32)
    for k in range(slots):
        own_waves = jnp.where(lane_row == k, wave_smem[k].astype(jnp.float32), own_waves)
    wave_send[...] = own_waves
    wave_recv[me] = own_waves

    spec_copy.wait()
    degree = lax.broadcasted_iota(jnp.int32, (1, degrees), 1)

    def slot_sums(k):
        offset = degree - wave_smem[k]
        kept = jnp.where(offset >= 0, 1.0, 0.0)
        flipped = jnp.where((offset & 1) == 0, kept, -kept)
        rows_in = spec[k].astype(jnp.float32)
        both = jnp.concatenate([rows_in * kept, rows_in * flipped], 0).astype(jnp.bfloat16)
        return jnp.dot(both, leg[k], preferred_element_type=jnp.float32)

    def target(i):
        to = lax.rem(me + i, devices)
        side = jnp.where(to >= half, 1, 0)
        block = jnp.where(to >= half, devices - 1 - to, to)
        return to, side, block

    def make_pair(s):
        leg_copy(s).wait()
        first = slot_sums(2 * s)
        second = slot_sums(2 * s + 1)
        for side in range(2):
            low = side * columns
            stacked = jnp.concatenate([first[low : low + columns], second[low : low + columns]], 0)
            turned[side] = stacked.T
        group = 4

        def pack(g, carry):
            for side in range(2):
                piece = turned[side, pl.ds(pl.multiple_of(g * group * rows, 8), group * rows), :]
                for i in range(group):
                    send[s, side, g * group + i] = piece[i * rows : (i + 1) * rows]
            return carry

        lax.fori_loop(0, half // group, pack, 0)

    def send_pair(s):
        def one(i, carry):
            to, side, block = target(i)
            pltpu.make_async_remote_copy(
                src_ref=send.at[s, side, block],
                dst_ref=recv.at[s, me],
                send_sem=send_sem.at[s],
                recv_sem=recv_sem.at[s],
                device_id=(lev, to),
                device_id_type=MESH,
            ).start()
            return carry

        lax.fori_loop(1, devices, one, 0)
        _, side, block = target(0)
        pltpu.make_async_copy(send.at[s, side, block], recv.at[s, me], recv_sem.at[s]).start()

    make_pair(0)
    pl.semaphore_wait(barrier, devices - 1)

    def send_waves(i, carry):
        pltpu.make_async_remote_copy(
            src_ref=wave_send,
            dst_ref=wave_recv.at[me],
            send_sem=wave_send_sem,
            recv_sem=wave_recv_sem,
            device_id=(lev, lax.rem(me + i, devices)),
            device_id_type=MESH,
        ).start()
        return carry

    lax.fori_loop(1, devices, send_waves, 0)
    send_pair(0)

    def later_pair(s, carry):
        make_pair(s)
        send_pair(s)
        return carry

    lax.fori_loop(1, pairs, later_pair, 0)

    others = pl.ds(0, devices - 1)
    pltpu.make_async_copy(wave_recv.at[others], wave_recv.at[others], wave_recv_sem).wait()

    waves = wave_recv[:, 0, :]
    step_units = waves - 20.0 * jnp.floor((waves + 0.5) * 0.05)
    step_angle = step_units * (2.0 * math.pi / 20.0)
    wave_trig[0] = waves
    wave_trig[1] = jnp.cos(step_angle)
    wave_trig[2] = jnp.sin(step_angle)
    acc[...] = jnp.zeros_like(acc)
    lane_id = lax.broadcasted_iota(jnp.int32, (devices, LANES), 1)
    lane_number = lane_id.astype(jnp.float32)

    def column(which, k):
        picked = jnp.where(lane_id == k, wave_trig[which], 0.0)
        return jnp.broadcast_to(jnp.sum(picked, axis=1, keepdims=True), (devices, LANES))

    def make_tables(s):
        for t in range(2):
            k = 2 * s + t
            wave = column(0, k)
            cos_step = column(1, k)
            sin_step = column(2, k)
            product = wave * lane_number
            turns = jnp.floor(product * (1.0 / NLON) + 0.5)
            angle = (product - turns * NLON) * (2.0 * math.pi / NLON)
            weight = jnp.where(wave == 0.0, 1.0, 2.0)
            cos_part = weight * jnp.cos(angle)
            sin_part = -weight * jnp.sin(angle)
            for q in range(NLON // LANES):
                at = slice(q * LANES, (q + 1) * LANES)
                for p, part in ((0, cos_part), (1, sin_part)):
                    low = (2 * t + p) * devices
                    high_bits = part.astype(jnp.bfloat16)
                    table_hi[low : low + devices, at] = high_bits
                    table_lo[low : low + devices, at] = (part - high_bits.astype(jnp.float32)).astype(jnp.bfloat16)
                cos_part, sin_part = (
                    cos_part * cos_step + sin_part * sin_step,
                    sin_part * cos_step - cos_part * sin_step,
                )

    all_rows = rows * levels

    def use_pair(s):
        for r in range(rows):
            tile = recv[s, :, r, :].T
            high_bits = tile.astype(jnp.bfloat16)
            low_bits = (tile - high_bits.astype(jnp.float32)).astype(jnp.bfloat16)
            at = pl.multiple_of(jnp.where(me >= half, rows - 1 - r, r) * levels, levels)
            for b in range(4):
                piece = slice(b * levels, (b + 1) * levels)
                across = slice(b * devices, (b + 1) * devices)
                xs[pl.ds(at, levels), across] = high_bits[piece]
                xs[pl.ds(at + all_rows, levels), across] = low_bits[piece]
        width = 512

        def block(j, carry):
            at = pl.ds(pl.multiple_of(j * width, width), width)
            main = jnp.dot(xs[...], table_hi[:, at], preferred_element_type=jnp.float32)
            rest = jnp.dot(xs[0:all_rows], table_lo[:, at], preferred_element_type=jnp.float32)
            acc[:, at] += main[0:all_rows] + (main[all_rows:] + rest)
            return carry

        lax.fori_loop(0, NLON // width, block, 0)

    def arrive(s, carry):
        make_tables(s)
        pltpu.make_async_copy(recv.at[s], recv.at[s], recv_sem.at[s]).wait()
        use_pair(s)
        return carry

    lax.fori_loop(0, pairs, arrive, 0)
    out_ref[...] = acc[...]

    def finish(s, carry):
        pltpu.make_async_copy(recv.at[s, others], recv.at[s, others], send_sem.at[s]).wait()
        return carry

    lax.fori_loop(0, pairs, finish, 0)
    pltpu.make_async_copy(wave_recv.at[others], wave_recv.at[others], wave_send_sem).wait()


def solution(mesh):
    devices = mesh.shape["wa"]

    def on_device(spectral, legendre, wavenumber):
        slots, degrees, parts, levels = spectral.shape
        north = legendre.shape[2]
        columns = parts * levels
        rows = 2 * north // devices
        pairs = slots // 2
        spec_rows = jnp.transpose(spectral, (0, 2, 3, 1)).reshape(slots, columns, degrees)
        dims = (devices, slots, degrees, north, columns, rows)
        gridded = pl.pallas_call(
            functools.partial(kernel, dims),
            out_shape=jax.ShapeDtypeStruct((rows * levels, NLON), jnp.float32),
            in_specs=[
                pl.BlockSpec(memory_space=pl.ANY),
                pl.BlockSpec(memory_space=pl.ANY),
                pl.BlockSpec(memory_space=pltpu.SMEM),
            ],
            out_specs=pl.BlockSpec(memory_space=pltpu.VMEM),
            scratch_shapes=[
                pltpu.VMEM((slots, columns, degrees), jnp.bfloat16),
                pltpu.VMEM((slots, degrees, north), jnp.bfloat16),
                pltpu.VMEM((2, north, LANES), jnp.float32),
                pltpu.VMEM((pairs, 2, devices // 2, rows, LANES), jnp.float32),
                pltpu.VMEM((pairs, devices, rows, LANES), jnp.float32),
                pltpu.VMEM((1, LANES), jnp.float32),
                pltpu.VMEM((devices, 1, LANES), jnp.float32),
                pltpu.VMEM((3, devices, LANES), jnp.float32),
                pltpu.VMEM((4 * devices, NLON), jnp.bfloat16),
                pltpu.VMEM((4 * devices, NLON), jnp.bfloat16),
                pltpu.VMEM((2 * rows * levels, 4 * devices), jnp.bfloat16),
                pltpu.VMEM((rows * levels, NLON), jnp.float32),
                pltpu.SemaphoreType.DMA,
                pltpu.SemaphoreType.DMA((pairs,)),
                pltpu.SemaphoreType.DMA,
                pltpu.SemaphoreType.DMA,
                pltpu.SemaphoreType.DMA((pairs,)),
                pltpu.SemaphoreType.DMA((pairs,)),
            ],
            compiler_params=pltpu.CompilerParams(
                collective_id=0, has_side_effects=True, vmem_limit_bytes=60 * 2**20
            ),
        )(spec_rows, legendre, wavenumber)
        return jnp.transpose(gridded.reshape(rows, levels, NLON), (0, 2, 1))

    return jax.shard_map(
        on_device,
        mesh=mesh,
        in_specs=(P("wa", None, None, "lev"), P("wa", None, None), P("wa")),
        out_specs=P("wa", None, "lev"),
        check_vma=False,
    )
```

```python
import functools
import math

import jax
import jax.numpy as jnp
from jax import lax
from jax.experimental import pallas as pl
from jax.experimental.pallas import tpu as pltpu
from jax.sharding import PartitionSpec as P

NLON = 2560
LANES = 128
MESH = pl.DeviceIdType.MESH
SIZES = (4, 8, 4)


def kernel(
    dims,
    spec_hbm,
    leg_hbm,
    wave_hbm,
    out_ref,
    spec,
    leg,
    turned,
    send,
    recv,
    wave_smem,
    wave_recv,
    wave_trig,
    table_hi,
    table_lo,
    xs,
    wave_sem,
    spec_sem,
    leg_sem,
    line_send_sem,
    line_recv_sem,
    plane_send_sem,
    plane_recv_sem,
    send_sem,
    recv_sem,
):
    sizes, slots, degrees, north, columns, rows = dims
    size_y, size_z, size_x = sizes
    devices = size_y * size_z * size_x
    plane = size_y * size_x
    quarter = size_z // 2
    pairs = slots // 2
    half = devices // 2
    levels = columns // 2
    lev = lax.axis_index("lev")
    me = lax.axis_index("wa")
    my_y = me // (size_z * size_x)
    my_z = lax.rem(me // size_x, size_z)
    my_x = lax.rem(me, size_x)

    def along_z(zslot):
        far, low = zslot // 2, lax.rem(zslot, 2)
        return jnp.where(low == 0, size_z // 2 - far, jnp.where(far == 0, 0, size_z // 2 + far))

    def in_plane(spot):
        dy = lax.rem(size_y // 2 + (size_y - 1) * (spot // size_x), size_y)
        dx = lax.rem(size_x // 2 + (size_x - 1) * lax.rem(spot, size_x), size_x)
        return dy, dx

    def device_at(dz, dy, dx):
        return (
            lax.rem(my_y + dy, size_y) * size_z + lax.rem(my_z + dz, size_z)
        ) * size_x + lax.rem(my_x + dx, size_x)

    own_spot = (size_y // 2) * size_x + size_x // 2
    own_place = own_spot * quarter + 1
    own_turn = 2 * own_spot + 1

    def place_of(zslot, spot):
        return (zslot // quarter) * half + spot * quarter + lax.rem(zslot, quarter)

    def copy_in(s):
        at = pl.ds(2 * s, 2)
        return (
            pltpu.make_async_copy(spec_hbm.at[at], spec.at[at], spec_sem.at[s]),
            pltpu.make_async_copy(leg_hbm.at[at], leg.at[at], leg_sem.at[s]),
        )

    wave_copy = pltpu.make_async_copy(wave_hbm, wave_smem, wave_sem)
    wave_copy.start()
    for copy in copy_in(0):
        copy.start()

    barrier = pltpu.get_barrier_semaphore()

    def greet(i, carry):
        pl.semaphore_signal(barrier, inc=1, device_id=(lev, lax.rem(me + i, devices)), device_id_type=MESH)
        return carry

    lax.fori_loop(1, devices, greet, 0)

    wave_copy.wait()
    lane_row = lax.broadcasted_iota(jnp.int32, (1, LANES), 1)
    own_waves = jnp.zeros((1, LANES), jnp.float32)
    for k in range(slots):
        own_waves = jnp.where(lane_row == k, wave_smem[k].astype(jnp.float32), own_waves)
    wave_recv[own_place] = own_waves

    degree = lax.broadcasted_iota(jnp.int32, (1, degrees), 1)

    def slot_sums(k):
        offset = degree - wave_smem[k]
        kept = jnp.where(offset >= 0, 1.0, 0.0)
        flipped = jnp.where((offset & 1) == 0, kept, -kept)
        rows_in = spec[k].astype(jnp.float32)
        both = jnp.concatenate([rows_in * kept, rows_in * flipped], 0).astype(jnp.bfloat16)
        return jnp.dot(both, leg[k], preferred_element_type=jnp.float32)

    def make_pair(s):
        first = slot_sums(2 * s)
        second = slot_sums(2 * s + 1)
        for side in range(2):
            low = side * columns
            stacked = jnp.concatenate([first[low : low + columns], second[low : low + columns]], 0)
            turned[side] = stacked.T
        group = 4

        def pack(g, carry):
            for side in range(2):
                piece = turned[side, pl.ds(pl.multiple_of(g * group * rows, 8), group * rows), :]
                for i in range(group):
                    send[s, side, g * group + i] = piece[i * rows : (i + 1) * rows]
            return carry

        lax.fori_loop(0, half // group, pack, 0)

    def own_block(to):
        return jnp.where(to >= half, 1, 0), jnp.where(to >= half, devices - 1 - to, to)

    def send_pair(s):
        def one(n, carry):
            turn = jnp.where(n >= own_turn, n + 1, n)
            far, rest = turn // (2 * plane), lax.rem(turn, 2 * plane)
            zslot, spot = 2 * far + lax.rem(rest, 2), rest // 2
            dy, dx = in_plane(spot)
            to = device_at(along_z(zslot), dy, dx)
            side, block = own_block(to)
            part = zslot // quarter
            pltpu.make_async_remote_copy(
                src_ref=send.at[s, side, block],
                dst_ref=recv.at[s, place_of(zslot, spot)],
                send_sem=send_sem.at[s],
                recv_sem=recv_sem.at[s, part],
                device_id=(lev, to),
                device_id_type=MESH,
            ).start()
            return carry

        lax.fori_loop(0, devices - 1, one, 0)
        side, block = own_block(me)
        pltpu.make_async_copy(send.at[s, side, block], recv.at[s, own_place], recv_sem.at[s, 0]).start()

    for copy in copy_in(0):
        copy.wait()
    for s in range(1, pairs):
        for copy in copy_in(s):
            copy.start()
    make_pair(0)
    out_ref[...] = jnp.zeros_like(out_ref)
    pl.semaphore_wait(barrier, devices - 1)

    def send_line(n, carry):
        zslot = jnp.where(n >= 1, n + 1, n)
        pltpu.make_async_remote_copy(
            src_ref=wave_recv.at[own_place],
            dst_ref=wave_recv.at[place_of(zslot, own_spot)],
            send_sem=line_send_sem,
            recv_sem=line_recv_sem,
            device_id=(lev, device_at(along_z(zslot), 0, 0)),
            device_id_type=MESH,
        ).start()
        return carry

    lax.fori_loop(0, size_z - 1, send_line, 0)
    send_pair(0)

    line_rows = wave_recv.at[pl.ds(0, size_z - 1)]
    pltpu.make_async_copy(line_rows, line_rows, line_recv_sem).wait()

    def send_plane(n, carry):
        spot = jnp.where(n >= own_spot, n + 1, n)
        dy, dx = in_plane(spot)
        for part in range(2):
            pltpu.make_async_remote_copy(
                src_ref=wave_recv.at[pl.ds(part * half + own_spot * quarter, quarter)],
                dst_ref=wave_recv.at[pl.ds(part * half + spot * quarter, quarter)],
                send_sem=plane_send_sem,
                recv_sem=plane_recv_sem,
                device_id=(lev, device_at(0, dy, dx)),
                device_id_type=MESH,
            ).start()
        return carry

    lax.fori_loop(0, plane - 1, send_plane, 0)

    def later_pair(s, carry):
        for copy in copy_in(s):
            copy.wait()
        make_pair(s)
        send_pair(s)
        return carry

    lax.fori_loop(1, pairs, later_pair, 0)

    plane_rows = wave_recv.at[pl.ds(0, size_z * (plane - 1))]
    pltpu.make_async_copy(plane_rows, plane_rows, plane_recv_sem).wait()

    waves = wave_recv[:, 0, :]
    step_units = waves - 20.0 * jnp.floor((waves + 0.5) * 0.05)
    step_angle = step_units * (2.0 * math.pi / 20.0)
    wave_trig[0] = waves
    wave_trig[1] = jnp.cos(step_angle)
    wave_trig[2] = jnp.sin(step_angle)
    lane_id = lax.broadcasted_iota(jnp.int32, (half, LANES), 1)
    lane_number = lane_id.astype(jnp.float32)

    def make_tables(s, part):
        first_row = pl.multiple_of(part * half, half)

        def column(which, k):
            picked = jnp.where(lane_id == k, wave_trig[which, pl.ds(first_row, half), :], 0.0)
            return jnp.broadcast_to(jnp.sum(picked, axis=1, keepdims=True), (half, LANES))

        for t in range(2):
            k = 2 * s + t
            wave = column(0, k)
            cos_step = column(1, k)
            sin_step = column(2, k)
            product = wave * lane_number
            turns = jnp.floor(product * (1.0 / NLON) + 0.5)
            angle = (product - turns * NLON) * (2.0 * math.pi / NLON)
            weight = jnp.where(wave == 0.0, 1.0, 2.0)
            cos_part = weight * jnp.cos(angle)
            sin_part = -weight * jnp.sin(angle)
            for q in range(NLON // LANES):
                at = slice(q * LANES, (q + 1) * LANES)
                for p, now in ((0, cos_part), (1, sin_part)):
                    low = (2 * t + p) * half
                    high_bits = now.astype(jnp.bfloat16)
                    table_hi[low : low + half, at] = high_bits
                    table_lo[low : low + half, at] = (now - high_bits.astype(jnp.float32)).astype(jnp.bfloat16)
                cos_part, sin_part = (
                    cos_part * cos_step + sin_part * sin_step,
                    sin_part * cos_step - cos_part * sin_step,
                )

    all_rows = rows * levels

    def use_part(s, part):
        for r in range(rows):
            tile = recv[s, pl.ds(part * half, half), r, :].T
            at = pl.multiple_of(jnp.where(me >= half, rows - 1 - r, r) * levels, levels)
            for t in range(2):
                low = 2 * t * levels
                piece = jnp.concatenate([tile[low : low + levels], tile[low + levels : low + 2 * levels]], 1)
                high_bits = piece.astype(jnp.bfloat16)
                low_bits = (piece - high_bits.astype(jnp.float32)).astype(jnp.bfloat16)
                across = slice(t * 2 * half, (t + 1) * 2 * half)
                xs[pl.ds(at, levels), across] = high_bits
                xs[pl.ds(at + all_rows, levels), across] = low_bits
        width = 512

        def block(j, carry):
            at = pl.ds(pl.multiple_of(j * width, width), width)
            main = jnp.dot(xs[...], table_hi[:, at], preferred_element_type=jnp.float32)
            rest = jnp.dot(xs[0:all_rows], table_lo[:, at], preferred_element_type=jnp.float32)
            out_ref[:, at] += main[0:all_rows] + (main[all_rows:] + rest)
            return carry

        lax.fori_loop(0, NLON // width, block, 0)

    def arrive(u, carry):
        s, part = u // 2, lax.rem(u, 2)
        make_tables(s, part)
        arrived = recv.at[s, pl.ds(part * half, half)]
        pltpu.make_async_copy(arrived, arrived, recv_sem.at[s, part]).wait()
        use_part(s, part)
        return carry

    def finish(s, carry):
        sent = recv.at[s, pl.ds(0, devices - 1)]
        pltpu.make_async_copy(sent, sent, send_sem.at[s]).wait()
        return carry

    lax.fori_loop(0, 2 * pairs, arrive, 0)
    lax.fori_loop(0, pairs, finish, 0)
    pltpu.make_async_copy(line_rows, line_rows, line_send_sem).wait()
    pltpu.make_async_copy(plane_rows, plane_rows, plane_send_sem).wait()


def solution(mesh):
    devices = mesh.shape["wa"]

    def on_device(spectral, legendre, wavenumber):
        slots, degrees, parts, levels = spectral.shape
        north = legendre.shape[2]
        columns = parts * levels
        rows = 2 * north // devices
        pairs = slots // 2
        half = devices // 2
        spec_rows = jnp.transpose(spectral, (0, 2, 3, 1)).reshape(slots, columns, degrees)
        dims = (SIZES, slots, degrees, north, columns, rows)
        gridded = pl.pallas_call(
            functools.partial(kernel, dims),
            out_shape=jax.ShapeDtypeStruct((rows * levels, NLON), jnp.float32),
            in_specs=[
                pl.BlockSpec(memory_space=pltpu.HBM),
                pl.BlockSpec(memory_space=pltpu.HBM),
                pl.BlockSpec(memory_space=pltpu.HBM),
            ],
            out_specs=pl.BlockSpec(memory_space=pltpu.VMEM),
            scratch_shapes=[
                pltpu.VMEM((slots, columns, degrees), jnp.bfloat16),
                pltpu.VMEM((slots, degrees, north), jnp.bfloat16),
                pltpu.VMEM((2, north, LANES), jnp.float32),
                pltpu.VMEM((pairs, 2, half, rows, LANES), jnp.float32),
                pltpu.VMEM((pairs, devices, rows, LANES), jnp.float32),
                pltpu.SMEM((slots,), jnp.int32),
                pltpu.VMEM((devices, 1, LANES), jnp.float32),
                pltpu.VMEM((3, devices, LANES), jnp.float32),
                pltpu.VMEM((4 * half, NLON), jnp.bfloat16),
                pltpu.VMEM((4 * half, NLON), jnp.bfloat16),
                pltpu.VMEM((2 * rows * levels, 4 * half), jnp.bfloat16),
                pltpu.SemaphoreType.DMA,
                pltpu.SemaphoreType.DMA((pairs,)),
                pltpu.SemaphoreType.DMA((pairs,)),
                pltpu.SemaphoreType.DMA,
                pltpu.SemaphoreType.DMA,
                pltpu.SemaphoreType.DMA,
                pltpu.SemaphoreType.DMA,
                pltpu.SemaphoreType.DMA((pairs,)),
                pltpu.SemaphoreType.DMA((pairs, 2)),
            ],
            compiler_params=pltpu.CompilerParams(
                collective_id=0, has_side_effects=True, vmem_limit_bytes=48 * 2**20
            ),
        )(
            pltpu.with_memory_space_constraint(spec_rows, pltpu.HBM),
            pltpu.with_memory_space_constraint(legendre, pltpu.HBM),
            pltpu.with_memory_space_constraint(wavenumber, pltpu.HBM),
        )
        return jnp.transpose(gridded.reshape(rows, levels, NLON), (0, 2, 1))

    return jax.shard_map(
        on_device,
        mesh=mesh,
        in_specs=(P("wa", None, None, "lev"), P("wa", None, None), P("wa")),
        out_specs=P("wa", None, "lev"),
        check_vma=False,
    )
```

```python
import functools
import math

import jax
import jax.numpy as jnp
from jax import lax
from jax.experimental import pallas as pl
from jax.experimental.pallas import tpu as pltpu
from jax.sharding import PartitionSpec as P

NLON = 2560
LANES = 128
MESH = pl.DeviceIdType.MESH
STEP = 4
LINE = 8
LINE_ORDER = (4, 3, 5, 2, 6, 1, 7, 0)


def kernel(
    dims,
    spec_hbm,
    leg_hbm,
    wave_hbm,
    out_ref,
    spec,
    leg,
    turned,
    send,
    recv,
    wave_smem,
    wave_recv,
    wave_trig,
    table_hi,
    table_lo,
    xs,
    wave_sem,
    spec_sem,
    leg_sem,
    line_send_sem,
    line_recv_sem,
    plane_send_sem,
    plane_recv_sem,
    send_sem,
    recv_sem,
):
    devices, slots, degrees, north, columns, rows = dims
    pairs = slots // 2
    half = devices // 2
    groups = devices // LINE
    levels = columns // 2
    lev = lax.axis_index("lev")
    me = lax.axis_index("wa")

    def target(m, k):
        return (me + (m // STEP * (LINE * STEP) + m % STEP + k * STEP)) & (devices - 1)

    def copy_row(src, dst, sends, receives, to):
        pltpu.make_async_remote_copy(
            src_ref=src,
            dst_ref=dst,
            send_sem=sends,
            recv_sem=receives,
            device_id=(lev, to),
            device_id_type=MESH,
        ).start()

    def copy_in(s):
        at = pl.ds(2 * s, 2)
        return (
            pltpu.make_async_copy(spec_hbm.at[at], spec.at[at], spec_sem.at[s]),
            pltpu.make_async_copy(leg_hbm.at[at], leg.at[at], leg_sem.at[s]),
        )

    wave_copy = pltpu.make_async_copy(wave_hbm, wave_smem, wave_sem)
    wave_copy.start()
    for copy in copy_in(0):
        copy.start()

    barrier = pltpu.get_barrier_semaphore()

    def greet(m, first):
        for k in range(first, LINE):
            pl.semaphore_signal(
                barrier, inc=1, device_id=(lev, (me + m * LINE + k) & (devices - 1)), device_id_type=MESH
            )

    greet(0, 1)

    def greet_line(m, carry):
        greet(m, 0)
        return carry

    lax.fori_loop(1, groups, greet_line, 0)

    wave_copy.wait()
    lane_row = lax.broadcasted_iota(jnp.int32, (1, LANES), 1)
    own_waves = jnp.zeros((1, LANES), jnp.float32)
    for k in range(slots):
        own_waves = jnp.where(lane_row == k, wave_smem[k].astype(jnp.float32), own_waves)
    wave_recv[0] = own_waves

    degree = lax.broadcasted_iota(jnp.int32, (1, degrees), 1)

    def slot_sums(k):
        offset = degree - wave_smem[k]
        kept = jnp.where(offset >= 0, 1.0, 0.0)
        flipped = jnp.where((offset & 1) == 0, kept, -kept)
        rows_in = spec[k].astype(jnp.float32)
        both = jnp.concatenate([rows_in * kept, rows_in * flipped], 0).astype(jnp.bfloat16)
        return jnp.dot(both, leg[k], preferred_element_type=jnp.float32)

    def make_pair(s):
        first = slot_sums(2 * s)
        second = slot_sums(2 * s + 1)
        for side in range(2):
            low = side * columns
            stacked = jnp.concatenate([first[low : low + columns], second[low : low + columns]], 0)
            turned[side] = stacked.T
        group = 4

        def pack(g, carry):
            for side in range(2):
                piece = turned[side, pl.ds(pl.multiple_of(g * group * rows, 8), group * rows), :]
                for i in range(group):
                    band = g * group + i
                    send[s, devices - 1 - band if side else band] = piece[i * rows : (i + 1) * rows]
            return carry

        lax.fori_loop(0, half // group, pack, 0)

    def send_group(s, m, part, first):
        for k in LINE_ORDER:
            if k >= first:
                to = target(m, k)
                copy_row(send.at[s, to], recv.at[s, m * LINE + k], send_sem.at[s], recv_sem.at[s, part], to)

    def send_pair(s):
        send_group(s, 0, 0, 1)
        for part in range(2):

            def one(m, carry):
                send_group(s, m, part, 0)
                return carry

            lax.fori_loop(max(1, part * groups // 2), (part + 1) * groups // 2, one, 0)
        pltpu.make_async_copy(send.at[s, me], recv.at[s, 0], recv_sem.at[s, 0]).start()

    for copy in copy_in(0):
        copy.wait()
    for s in range(1, pairs):
        for copy in copy_in(s):
            copy.start()
    make_pair(0)
    out_ref[...] = jnp.zeros_like(out_ref)
    pl.semaphore_wait(barrier, devices - 1)

    for k in range(1, LINE):
        copy_row(wave_recv.at[0], wave_recv.at[k], line_send_sem, line_recv_sem, target(0, k))
    send_pair(0)

    line_rows = wave_recv.at[pl.ds(0, LINE - 1)]
    pltpu.make_async_copy(line_rows, line_rows, line_recv_sem).wait()

    def send_plane(m, carry):
        rows_out = wave_recv.at[pl.ds(m * LINE, LINE)]
        copy_row(wave_recv.at[pl.ds(0, LINE)], rows_out, plane_send_sem, plane_recv_sem, target(m, 0))
        return carry

    lax.fori_loop(1, groups, send_plane, 0)

    def later_pair(s, carry):
        for copy in copy_in(s):
            copy.wait()
        make_pair(s)
        send_pair(s)
        return carry

    lax.fori_loop(1, pairs, later_pair, 0)

    plane_rows = wave_recv.at[pl.ds(0, devices - LINE)]
    pltpu.make_async_copy(plane_rows, plane_rows, plane_recv_sem).wait()

    waves = wave_recv[:, 0, :]
    step_units = waves - 20.0 * jnp.floor((waves + 0.5) * 0.05)
    step_angle = step_units * (2.0 * math.pi / 20.0)
    wave_trig[0] = waves
    wave_trig[1] = jnp.cos(step_angle)
    wave_trig[2] = jnp.sin(step_angle)
    lane_id = lax.broadcasted_iota(jnp.int32, (half, LANES), 1)
    lane_number = lane_id.astype(jnp.float32)

    def make_tables(s, part):
        first_row = pl.multiple_of(part * half, half)

        def column(which, k):
            picked = jnp.where(lane_id == k, wave_trig[which, pl.ds(first_row, half), :], 0.0)
            return jnp.broadcast_to(jnp.sum(picked, axis=1, keepdims=True), (half, LANES))

        for t in range(2):
            k = 2 * s + t
            wave = column(0, k)
            cos_step = column(1, k)
            sin_step = column(2, k)
            product = wave * lane_number
            turns = jnp.floor(product * (1.0 / NLON) + 0.5)
            angle = (product - turns * NLON) * (2.0 * math.pi / NLON)
            weight = jnp.where(wave == 0.0, 1.0, 2.0)
            cos_part = weight * jnp.cos(angle)
            sin_part = -weight * jnp.sin(angle)
            for q in range(NLON // LANES):
                at = slice(q * LANES, (q + 1) * LANES)
                for p, now in ((0, cos_part), (1, sin_part)):
                    low = (2 * t + p) * half
                    high_bits = now.astype(jnp.bfloat16)
                    table_hi[low : low + half, at] = high_bits
                    table_lo[low : low + half, at] = (now - high_bits.astype(jnp.float32)).astype(jnp.bfloat16)
                cos_part, sin_part = (
                    cos_part * cos_step + sin_part * sin_step,
                    sin_part * cos_step - cos_part * sin_step,
                )

    all_rows = rows * levels

    def use_part(s, part):
        for r in range(rows):
            tile = recv[s, pl.ds(part * half, half), r, :].T
            at = pl.multiple_of(jnp.where(me >= half, rows - 1 - r, r) * levels, levels)
            for t in range(2):
                low = 2 * t * levels
                piece = jnp.concatenate([tile[low : low + levels], tile[low + levels : low + 2 * levels]], 1)
                high_bits = piece.astype(jnp.bfloat16)
                low_bits = (piece - high_bits.astype(jnp.float32)).astype(jnp.bfloat16)
                across = slice(t * 2 * half, (t + 1) * 2 * half)
                xs[pl.ds(at, levels), across] = high_bits
                xs[pl.ds(at + all_rows, levels), across] = low_bits
        width = 512

        def block(j, carry):
            at = pl.ds(pl.multiple_of(j * width, width), width)
            main = jnp.dot(xs[...], table_hi[:, at], preferred_element_type=jnp.float32)
            rest = jnp.dot(xs[0:all_rows], table_lo[:, at], preferred_element_type=jnp.float32)
            out_ref[:, at] += main[0:all_rows] + (main[all_rows:] + rest)
            return carry

        lax.fori_loop(0, NLON // width, block, 0)

    def arrive(u, carry):
        s, part = u // 2, lax.rem(u, 2)
        make_tables(s, part)
        arrived = recv.at[s, pl.ds(part * half, half)]
        pltpu.make_async_copy(arrived, arrived, recv_sem.at[s, part]).wait()
        use_part(s, part)
        return carry

    def finish(s, carry):
        sent = recv.at[s, pl.ds(0, devices - 1)]
        pltpu.make_async_copy(sent, sent, send_sem.at[s]).wait()
        return carry

    lax.fori_loop(0, 2 * pairs, arrive, 0)
    lax.fori_loop(0, pairs, finish, 0)
    pltpu.make_async_copy(line_rows, line_rows, line_send_sem).wait()
    pltpu.make_async_copy(plane_rows, plane_rows, plane_send_sem).wait()


def solution(mesh):
    devices = mesh.shape["wa"]

    def on_device(spectral, legendre, wavenumber):
        slots, degrees, parts, levels = spectral.shape
        north = legendre.shape[2]
        columns = parts * levels
        rows = 2 * north // devices
        pairs = slots // 2
        half = devices // 2
        spec_rows = jnp.transpose(spectral, (0, 2, 3, 1)).reshape(slots, columns, degrees)
        dims = (devices, slots, degrees, north, columns, rows)
        gridded = pl.pallas_call(
            functools.partial(kernel, dims),
            out_shape=jax.ShapeDtypeStruct((rows * levels, NLON), jnp.float32),
            in_specs=[
                pl.BlockSpec(memory_space=pltpu.HBM),
                pl.BlockSpec(memory_space=pltpu.HBM),
                pl.BlockSpec(memory_space=pltpu.HBM),
            ],
            out_specs=pl.BlockSpec(memory_space=pltpu.VMEM),
            scratch_shapes=[
                pltpu.VMEM((slots, columns, degrees), jnp.bfloat16),
                pltpu.VMEM((slots, degrees, north), jnp.bfloat16),
                pltpu.VMEM((2, north, LANES), jnp.float32),
                pltpu.VMEM((pairs, devices, rows, LANES), jnp.float32),
                pltpu.VMEM((pairs, devices, rows, LANES), jnp.float32),
                pltpu.SMEM((slots,), jnp.int32),
                pltpu.VMEM((devices, 1, LANES), jnp.float32),
                pltpu.VMEM((3, devices, LANES), jnp.float32),
                pltpu.VMEM((4 * half, NLON), jnp.bfloat16),
                pltpu.VMEM((4 * half, NLON), jnp.bfloat16),
                pltpu.VMEM((2 * rows * levels, 4 * half), jnp.bfloat16),
                pltpu.SemaphoreType.DMA,
                pltpu.SemaphoreType.DMA((pairs,)),
                pltpu.SemaphoreType.DMA((pairs,)),
                pltpu.SemaphoreType.DMA,
                pltpu.SemaphoreType.DMA,
                pltpu.SemaphoreType.DMA,
                pltpu.SemaphoreType.DMA,
                pltpu.SemaphoreType.DMA((pairs,)),
                pltpu.SemaphoreType.DMA((pairs, 2)),
            ],
            compiler_params=pltpu.CompilerParams(
                collective_id=0, has_side_effects=True, vmem_limit_bytes=48 * 2**20
            ),
        )(
            pltpu.with_memory_space_constraint(spec_rows, pltpu.HBM),
            pltpu.with_memory_space_constraint(legendre, pltpu.HBM),
            pltpu.with_memory_space_constraint(wavenumber, pltpu.HBM),
        )
        return jnp.transpose(gridded.reshape(rows, levels, NLON), (0, 2, 1))

    return jax.shard_map(
        on_device,
        mesh=mesh,
        in_specs=(P("wa", None, None, "lev"), P("wa", None, None), P("wa")),
        out_specs=P("wa", None, "lev"),
        check_vma=False,
    )
```

```python
import functools
import math

import jax
import jax.numpy as jnp
from jax import lax
from jax.experimental import pallas as pl
from jax.experimental.pallas import tpu as pltpu
from jax.sharding import PartitionSpec as P

NLON = 2560
LANES = 128
MESH = pl.DeviceIdType.MESH
STEP = 4
LINE = 8
LINE_ORDER = (4, 3, 5, 2, 6, 1, 7, 0)


def kernel(
    dims,
    spec_hbm,
    leg_hbm,
    wave_hbm,
    out_ref,
    spec,
    leg,
    turned,
    send,
    recv,
    wave_smem,
    wave_recv,
    wave_trig,
    table,
    sign,
    xs,
    wave_sem,
    spec_sem,
    leg_sem,
    line_send_sem,
    line_recv_sem,
    plane_send_sem,
    plane_recv_sem,
    send_sem,
    recv_sem,
):
    devices, slots, degrees, north, columns, rows = dims
    pairs = slots // 2
    half = devices // 2
    groups = devices // LINE
    levels = columns // 2
    lev = lax.axis_index("lev")
    me = lax.axis_index("wa")

    def target(m, k):
        return (me + (m // STEP * (LINE * STEP) + m % STEP + k * STEP)) & (devices - 1)

    def copy_row(src, dst, sends, receives, to):
        pltpu.make_async_remote_copy(
            src_ref=src,
            dst_ref=dst,
            send_sem=sends,
            recv_sem=receives,
            device_id=(lev, to),
            device_id_type=MESH,
        ).start()

    def copy_in(s):
        at = pl.ds(2 * s, 2)
        return (
            pltpu.make_async_copy(spec_hbm.at[at], spec.at[at], spec_sem.at[s]),
            pltpu.make_async_copy(leg_hbm.at[at], leg.at[at], leg_sem.at[s]),
        )

    wave_copy = pltpu.make_async_copy(wave_hbm, wave_smem, wave_sem)
    wave_copy.start()
    for copy in copy_in(0):
        copy.start()

    barrier = pltpu.get_barrier_semaphore()

    def greet(m, first):
        for k in range(first, LINE):
            pl.semaphore_signal(
                barrier, inc=1, device_id=(lev, (me + m * LINE + k) & (devices - 1)), device_id_type=MESH
            )

    greet(0, 1)

    def greet_line(m, carry):
        greet(m, 0)
        return carry

    lax.fori_loop(1, groups, greet_line, 0)

    wave_copy.wait()
    lane_row = lax.broadcasted_iota(jnp.int32, (1, LANES), 1)
    own_waves = jnp.zeros((1, LANES), jnp.float32)
    for k in range(slots):
        own_waves = jnp.where(lane_row == k, wave_smem[k].astype(jnp.float32), own_waves)
    wave_recv[0] = own_waves

    degree = lax.broadcasted_iota(jnp.int32, (1, degrees), 1)

    def slot_sums(k):
        offset = degree - wave_smem[k]
        kept = jnp.where(offset >= 0, 1.0, 0.0)
        flipped = jnp.where((offset & 1) == 0, kept, -kept)
        rows_in = spec[k].astype(jnp.float32)
        both = jnp.concatenate([rows_in * kept, rows_in * flipped], 0).astype(jnp.bfloat16)
        return jnp.dot(both, leg[k], preferred_element_type=jnp.float32)

    def make_pair(s):
        first = slot_sums(2 * s)
        second = slot_sums(2 * s + 1)
        for side in range(2):
            low = side * columns
            stacked = jnp.concatenate([first[low : low + columns], second[low : low + columns]], 0)
            turned[side] = stacked.T
        group = 4

        def pack(g, carry):
            for side in range(2):
                piece = turned[side, pl.ds(pl.multiple_of(g * group * rows, 8), group * rows), :]
                for i in range(group):
                    band = g * group + i
                    send[s, devices - 1 - band if side else band] = piece[i * rows : (i + 1) * rows]
            return carry

        lax.fori_loop(0, half // group, pack, 0)

    def send_group(s, m, part, first):
        for k in LINE_ORDER:
            if k >= first:
                to = target(m, k)
                copy_row(send.at[s, to], recv.at[s, m * LINE + k], send_sem.at[s], recv_sem.at[s, part], to)

    def send_pair(s):
        send_group(s, 0, 0, 1)
        for part in range(2):

            def one(m, carry):
                send_group(s, m, part, 0)
                return carry

            lax.fori_loop(max(1, part * groups // 2), (part + 1) * groups // 2, one, 0)
        pltpu.make_async_copy(send.at[s, me], recv.at[s, 0], recv_sem.at[s, 0]).start()

    for copy in copy_in(0):
        copy.wait()
    for s in range(1, pairs):
        for copy in copy_in(s):
            copy.start()
    make_pair(0)
    out_ref[...] = jnp.zeros_like(out_ref)
    pl.semaphore_wait(barrier, devices - 1)

    for k in range(1, LINE):
        copy_row(wave_recv.at[0], wave_recv.at[k], line_send_sem, line_recv_sem, target(0, k))
    send_pair(0)

    line_rows = wave_recv.at[pl.ds(0, LINE - 1)]
    pltpu.make_async_copy(line_rows, line_rows, line_recv_sem).wait()

    def send_plane(m, carry):
        rows_out = wave_recv.at[pl.ds(m * LINE, LINE)]
        copy_row(wave_recv.at[pl.ds(0, LINE)], rows_out, plane_send_sem, plane_recv_sem, target(m, 0))
        return carry

    lax.fori_loop(1, groups, send_plane, 0)

    def later_pair(s, carry):
        for copy in copy_in(s):
            copy.wait()
        make_pair(s)
        send_pair(s)
        return carry

    lax.fori_loop(1, pairs, later_pair, 0)

    plane_rows = wave_recv.at[pl.ds(0, devices - LINE)]
    pltpu.make_async_copy(plane_rows, plane_rows, plane_recv_sem).wait()

    waves = wave_recv[:, 0, :]
    step_units = waves - 20.0 * jnp.floor((waves + 0.5) * 0.05)
    step_angle = step_units * (2.0 * math.pi / 20.0)
    wave_trig[0] = waves
    wave_trig[1] = jnp.cos(step_angle)
    wave_trig[2] = jnp.sin(step_angle)
    wave_trig[3] = 1.0 - 2.0 * (waves - 2.0 * jnp.floor(waves * 0.5))
    lane_id = lax.broadcasted_iota(jnp.int32, (half, LANES), 1)
    lane_number = lane_id.astype(jnp.float32)

    all_rows = rows * levels
    deep = 4 * half

    def make_tables(s, part):
        first_row = pl.multiple_of(part * half, half)

        def column(which, k):
            picked = jnp.where(lane_id == k, wave_trig[which, pl.ds(first_row, half), :], 0.0)
            return jnp.broadcast_to(jnp.sum(picked, axis=1, keepdims=True), (half, LANES))

        signs = jnp.where(lane_id < LANES // 2, column(3, 2 * s), column(3, 2 * s + 1))
        sign[...] = signs.T
        for t in range(2):
            k = 2 * s + t
            wave = column(0, k)
            cos_step = column(1, k)
            sin_step = column(2, k)
            product = wave * lane_number
            turns = jnp.floor(product * (1.0 / NLON) + 0.5)
            angle = (product - turns * NLON) * (2.0 * math.pi / NLON)
            weight = jnp.where(wave == 0.0, 1.0, 2.0)
            cos_part = weight * jnp.cos(angle)
            sin_part = -weight * jnp.sin(angle)
            for q in range(NLON // 2 // LANES):
                at = slice(q * LANES, (q + 1) * LANES)
                for p, now in ((0, cos_part), (1, sin_part)):
                    low = (2 * t + p) * half
                    high_bits = now.astype(jnp.bfloat16)
                    low_bits = (now - high_bits.astype(jnp.float32)).astype(jnp.bfloat16)
                    table[low : low + half, at] = high_bits
                    table[deep + low : deep + low + half, at] = low_bits
                cos_part, sin_part = (
                    cos_part * cos_step + sin_part * sin_step,
                    sin_part * cos_step - cos_part * sin_step,
                )


    def use_part(s, part):
        for r in range(rows):
            tile = recv[s, pl.ds(part * half, half), r, :].T
            at = pl.multiple_of(jnp.where(me >= half, rows - 1 - r, r) * levels, levels)
            for t in range(2):
                low = 2 * t * levels
                piece = jnp.concatenate([tile[low : low + levels], tile[low + levels : low + 2 * levels]], 1)
                high_bits = piece.astype(jnp.bfloat16)
                low_bits = (piece - high_bits.astype(jnp.float32)).astype(jnp.bfloat16)
                turn = sign[low : low + levels].astype(jnp.bfloat16)
                turn = jnp.concatenate([turn, turn], 1)
                for i, bits in enumerate((high_bits, high_bits, low_bits)):
                    across = slice(i * deep + t * 2 * half, i * deep + (t + 1) * 2 * half)
                    xs[pl.ds(at, levels), across] = bits
                    xs[pl.ds(at + all_rows, levels), across] = bits * turn
        total = jnp.dot(xs[:, 0 : 2 * deep], table[...], preferred_element_type=jnp.float32)
        total += jnp.dot(xs[:, 2 * deep :], table[0:deep], preferred_element_type=jnp.float32)
        out_ref[:, 0 : NLON // 2] += total[0:all_rows]
        out_ref[:, NLON // 2 :] += total[all_rows:]

    def arrive(u, carry):
        s, part = u // 2, lax.rem(u, 2)
        make_tables(s, part)
        arrived = recv.at[s, pl.ds(part * half, half)]
        pltpu.make_async_copy(arrived, arrived, recv_sem.at[s, part]).wait()
        use_part(s, part)
        return carry

    def finish(s, carry):
        sent = recv.at[s, pl.ds(0, devices - 1)]
        pltpu.make_async_copy(sent, sent, send_sem.at[s]).wait()
        return carry

    lax.fori_loop(0, 2 * pairs, arrive, 0)
    lax.fori_loop(0, pairs, finish, 0)
    pltpu.make_async_copy(line_rows, line_rows, line_send_sem).wait()
    pltpu.make_async_copy(plane_rows, plane_rows, plane_send_sem).wait()


def solution(mesh):
    devices = mesh.shape["wa"]

    def on_device(spectral, legendre, wavenumber):
        slots, degrees, parts, levels = spectral.shape
        north = legendre.shape[2]
        columns = parts * levels
        rows = 2 * north // devices
        pairs = slots // 2
        half = devices // 2
        spec_rows = jnp.transpose(spectral, (0, 2, 3, 1)).reshape(slots, columns, degrees)
        dims = (devices, slots, degrees, north, columns, rows)
        gridded = pl.pallas_call(
            functools.partial(kernel, dims),
            out_shape=jax.ShapeDtypeStruct((rows * levels, NLON), jnp.float32),
            in_specs=[
                pl.BlockSpec(memory_space=pltpu.HBM),
                pl.BlockSpec(memory_space=pltpu.HBM),
                pl.BlockSpec(memory_space=pltpu.HBM),
            ],
            out_specs=pl.BlockSpec(memory_space=pltpu.VMEM),
            scratch_shapes=[
                pltpu.VMEM((slots, columns, degrees), jnp.bfloat16),
                pltpu.VMEM((slots, degrees, north), jnp.bfloat16),
                pltpu.VMEM((2, north, LANES), jnp.float32),
                pltpu.VMEM((pairs, devices, rows, LANES), jnp.float32),
                pltpu.VMEM((pairs, devices, rows, LANES), jnp.float32),
                pltpu.SMEM((slots,), jnp.int32),
                pltpu.VMEM((devices, 1, LANES), jnp.float32),
                pltpu.VMEM((4, devices, LANES), jnp.float32),
                pltpu.VMEM((8 * half, NLON // 2), jnp.bfloat16),
                pltpu.VMEM((LANES, half), jnp.float32),
                pltpu.VMEM((2 * rows * levels, 12 * half), jnp.bfloat16),
                pltpu.SemaphoreType.DMA,
                pltpu.SemaphoreType.DMA((pairs,)),
                pltpu.SemaphoreType.DMA((pairs,)),
                pltpu.SemaphoreType.DMA,
                pltpu.SemaphoreType.DMA,
                pltpu.SemaphoreType.DMA,
                pltpu.SemaphoreType.DMA,
                pltpu.SemaphoreType.DMA((pairs,)),
                pltpu.SemaphoreType.DMA((pairs, 2)),
            ],
            compiler_params=pltpu.CompilerParams(
                collective_id=0, has_side_effects=True, vmem_limit_bytes=48 * 2**20
            ),
        )(
            pltpu.with_memory_space_constraint(spec_rows, pltpu.HBM),
            pltpu.with_memory_space_constraint(legendre, pltpu.HBM),
            pltpu.with_memory_space_constraint(wavenumber, pltpu.HBM),
        )
        return jnp.transpose(gridded.reshape(rows, levels, NLON), (0, 2, 1))

    return jax.shard_map(
        on_device,
        mesh=mesh,
        in_specs=(P("wa", None, None, "lev"), P("wa", None, None), P("wa")),
        out_specs=P("wa", None, "lev"),
        check_vma=False,
    )
```
